128 devices in a mesh: vocab: 64 (over x, y, z), dp: 2 (over core).
Axes of the slice: x: 4, y: 4, z: 4, core: 2. Of those that a mesh axis runs over, the one named last changes fastest.
Arguments:
- embed_table: bfloat16 [65536, 4096], P('vocab'), may hold values from -3 to 3
- token_ids: int32 [2, 65536], P('dp', 'vocab'), may hold values from 0 to 65535, as said below
- grad_rows: bfloat16 [2, 65536, 4096], P('dp', 'vocab'), may hold values from -12 to 12
Outputs:
- updated: bfloat16 [65536, 4096], P('vocab', 'dp')
- grad_rms: float32 [1], replicated
The draws below stay inside these ranges and needn't reach their ends.
Inputs may be any that keep to these rules, and one draw needn't show every extreme that they name: `token_ids`: rows are read cyclically: row r stands for every r + k * 65536. The window of vocab index v (tokens v * 1024 to (v + 1) * 1024 - 1 of a replica) holds ids that, read as the cyclic representatives from v * 1024 - 256 to (v + 1) * 1024 + 255, rise (never fall) along its tokens; both ends are reached in some window. Only its first 128 and last 128 tokens may lie outside rows v * 1024 to (v + 1) * 1024 - 1 (so read), the first ones below, the last ones above; in every window its first token lies below and its last above, in some window all first 128 lie below, in some all last 128 above.
All inputs are finite; a program needn't handle non-finite values.
Results may differ from the reference program's by a relative error of at most 0.002.
Values may be sent and summed in bfloat16 or wider, within the bound.
No kernel may reach another device: no remote copies, remote signals or barrier semaphores. Data moves between devices by JAX's collectives and lax.ppermute only.
A program may use at most 128 MiB of HBM per device.

```python
import jax
import jax.numpy as jnp

D = 4096
ROWS_DEV = 1024
EDGE = 256
TOK_EDGE = 128
TOK_DEV = 1024
VOCAB = 65536
TOKENS = 65536
N_DP = 2


def draw_replica(key):
    windows = TOKENS // TOK_DEV
    key_above, key_below, key_first, key_middle, key_last = jax.random.split(key, 5)
    below = jax.random.randint(key_below, (windows,), 1, EDGE + 1)
    below = below.at[1].set(EDGE)
    above = jax.random.randint(key_above, (windows,), 1, EDGE + 1)
    above = above.at[windows - 1].set(EDGE)
    reach_up = jnp.roll(above, -1)
    device_ids = jnp.arange(windows, dtype=jnp.int32)
    starts = device_ids * ROWS_DEV
    first_low = starts - below
    first_high = jnp.where(device_ids == 1, starts, starts + ROWS_DEV // 2)
    last_low = jnp.where(device_ids == windows - 2, starts + ROWS_DEV, starts + ROWS_DEV - ROWS_DEV // 2)
    last_high = starts + ROWS_DEV + reach_up
    first_group = jax.random.randint(key_first, (windows, TOK_EDGE), first_low[:, None], first_high[:, None])
    first_group = first_group.at[:, 0].set(first_low)
    middle_group = jax.random.randint(key_middle, (windows, TOK_DEV - 2 * TOK_EDGE), starts[:, None], starts[:, None] + ROWS_DEV)
    last_group = jax.random.randint(key_last, (windows, TOK_EDGE), last_low[:, None], last_high[:, None])
    last_group = last_group.at[:, TOK_EDGE - 1].set(last_high - 1)
    window_ids = jnp.sort(jnp.concatenate([first_group, middle_group, last_group], axis=1), axis=1)
    window_ids = jnp.mod(window_ids, windows * ROWS_DEV)
    return window_ids.reshape(windows * TOK_DEV).astype(jnp.int32)


def draw_token_ids(key, part):
    replica_keys = jax.random.split(jax.random.fold_in(key, 11), N_DP)
    return jnp.stack([draw_replica(replica_keys[index]) for index in range(N_DP)])


def draw_grad_rows(key, part):
    windows = TOKENS // TOK_DEV
    key_base = jax.random.fold_in(jax.random.fold_in(key, 23), 0)
    key_window = jax.random.fold_in(jax.random.fold_in(key, 23), 3)
    values = jax.random.normal(key_base, (N_DP, TOKENS, D), jnp.float32)
    window_scale = jnp.exp(jax.random.uniform(key_window, (N_DP, windows, 1), jnp.float32, -1.2, 1.2))
    window_scale = jnp.repeat(window_scale, TOK_DEV, axis=1)
    values = window_scale * values
    return jnp.clip(values, -12.0, 12.0).astype(jnp.bfloat16)


def block_levels(own_key, extent, shards, least, high):
    gain = 1.0
    for axis_at, blocks in shards:
        steps = jax.random.uniform(jax.random.fold_in(jax.random.fold_in(own_key, 6), axis_at), (blocks,), jnp.float32, least / len(shards), high / len(shards))
        gain = gain * jnp.repeat(jnp.exp(steps), extent[axis_at] // blocks).reshape((-1,) + (1,) * (len(extent) - 1 - axis_at))
    return gain


def centred(own_key, shape, width, limit, cuts=(), kind=jnp.bfloat16):
    entries = width * jax.random.normal(own_key, shape, jnp.float32)
    if cuts:
        entries = entries * block_levels(own_key, shape, cuts, -0.22, 0.18)
    return jnp.clip(entries, -limit, limit).astype(kind)


def setup_inputs(seed: int = 0) -> dict:
    streams_of = jax.random.split(jax.random.key(seed), 4)
    embed_table = centred(streams_of[0], (VOCAB, D), 0.5, 3.0, ((0, 64),))
    token_ids = draw_token_ids(jax.random.fold_in(streams_of[3], 71), 0)
    grad_rows = draw_grad_rows(jax.random.fold_in(streams_of[3], 71), 0)
    return {"embed_table": embed_table, "token_ids": token_ids, "grad_rows": grad_rows}


step_rate = 0.5
norm_limit = 1.0

def reference(embed_table, token_ids, grad_rows):
    gradient = jnp.zeros((VOCAB, D), jnp.float32)
    for replica in range(N_DP):
        gradient = gradient + jax.ops.segment_sum(grad_rows[replica].astype(jnp.float32), token_ids[replica], num_segments=VOCAB)
    grad_rms = jnp.sqrt(jnp.sum(gradient * gradient) / (VOCAB * D))
    clip_scale = 1.0 / jnp.maximum(1.0, grad_rms / norm_limit)
    updated = (embed_table.astype(jnp.float32) - step_rate * clip_scale * gradient).astype(jnp.bfloat16)
    return (updated, jnp.reshape(grad_rms, (1,)))
```

```python
import functools

import jax
import jax.numpy as jnp
from jax import lax
from jax.experimental import pallas as pl
from jax.experimental.pallas import tpu as pltpu
from jax.sharding import Mesh
from jax.sharding import PartitionSpec as P

VOCAB = ("vocab_0", "vocab_1", "vocab_2")
VOCAB_DP = ("vocab_0", "vocab_1", "vocab_2", "dp")
TOK_EDGE = 128
EDGE = 256

step_rate = 0.5
norm_limit = 1.0


MIB = 1 << 20


def own_index():
    vocab = 0
    for name in VOCAB:
        vocab = vocab * lax.axis_size(name) + lax.axis_index(name)
    return vocab, lax.axis_index("dp")


def in_vmem(value):
    return pltpu.with_memory_space_constraint(value, pltpu.VMEM)


def in_hbm(value):
    return pltpu.with_memory_space_constraint(value, pltpu.HBM)


def any_spec():
    return pl.BlockSpec(memory_space=pltpu.HBM)


def vmem_spec():
    return pl.BlockSpec(memory_space=pltpu.VMEM)


def pack_edges(grad_rows):
    tokens, width = grad_rows.shape
    half = width // 2

    def kernel(rows, x_same, x_cross, y_same, y_cross, sems):
        vocab, core = own_index()
        odd = vocab % 2
        last = tokens - TOK_EDGE
        x_at = pl.multiple_of((1 - odd) * last, TOK_EDGE)
        y_at = pl.multiple_of(odd * last, TOK_EDGE)
        own = pl.multiple_of(core * half, half)
        other = pl.multiple_of((1 - core) * half, half)
        copies = []
        for k, (at, columns, out) in enumerate(
            ((y_at, own, y_same), (x_at, own, x_same), (y_at, other, y_cross), (x_at, other, x_cross))
        ):
            copies.append(
                pltpu.make_async_copy(
                    rows.at[pl.ds(at, TOK_EDGE), pl.ds(columns, half)], out, sems.at[k]
                )
            )
        for copy in copies:
            copy.start()
        for copy in copies:
            copy.wait()

    piece = pltpu.VMEM((TOK_EDGE, half), grad_rows.dtype)
    return pl.pallas_call(
        kernel,
        out_shape=[piece] * 4,
        in_specs=[any_spec()],
        out_specs=[vmem_spec()] * 4,
        scratch_shapes=[pltpu.SemaphoreType.DMA((4,))],
        compiler_params=pltpu.CompilerParams(vmem_limit_bytes=6 * MIB),
        name="pack_edges",
    )(in_hbm(grad_rows))


def pack_swap(grad_rows):
    tokens, width = grad_rows.shape
    half = width // 2
    parts = 4

    def kernel(rows, out, sems):
        _, core = own_index()
        other = pl.multiple_of((1 - core) * half, half)
        step = tokens // parts
        copies = [
            pltpu.make_async_copy(
                rows.at[pl.ds(k * step, step), pl.ds(other, half)],
                out.at[pl.ds(k * step, step), :],
                sems.at[k],
            )
            for k in range(parts)
        ]
        for copy in copies:
            copy.start()
        for copy in copies:
            copy.wait()

    return pl.pallas_call(
        kernel,
        out_shape=pltpu.VMEM((tokens, half), grad_rows.dtype),
        in_specs=[any_spec()],
        out_specs=vmem_spec(),
        scratch_shapes=[pltpu.SemaphoreType.DMA((parts,))],
        compiler_params=pltpu.CompilerParams(vmem_limit_bytes=6 * MIB),
        name="pack_swap",
    )(in_hbm(grad_rows))


def local_gradient(grad_rows, swapped_rows, own_ids, swapped_ids, embed_table, vocab_rows):
    tokens, width = grad_rows.shape
    rows_dev = embed_table.shape[0]
    half = width // 2
    block = 256
    lanes = 512

    def kernel(rows, far_rows, ids, far_ids, table, grad, own_table, squares, own_rows, hot, far_hot, sems):
        vocab, core = own_index()
        own = pl.multiple_of(core * half, half)
        copies = [
            pltpu.make_async_copy(
                rows.at[:, pl.ds(own + k * lanes, lanes)], own_rows.at[:, pl.ds(k * lanes, lanes)], sems.at[k]
            )
            for k in range(half // lanes)
        ]
        for copy in copies:
            copy.start()
        table_copy = pltpu.make_async_copy(table.at[:, pl.ds(own, half)], own_table, sems.at[half // lanes])
        table_copy.start()
        start = vocab * rows_dev
        for one_hot, token_ids in ((hot, ids), (far_hot, far_ids)):
            local = jnp.bitwise_and(token_ids[...] - start, vocab_rows - 1)
            for k in range(rows_dev // block):
                at = lax.broadcasted_iota(jnp.int32, (block, tokens), 0) + k * block
                one_hot[pl.ds(k * block, block), :] = jnp.where(at == local, 1.0, 0.0).astype(jnp.bfloat16)
        total = jnp.zeros((1, lanes), jnp.float32)
        for c in range(half // lanes):
            copies[c].wait()
            for r in range(rows_dev // block):
                part = jnp.dot(
                    hot[pl.ds(r * block, block), :],
                    own_rows[:, pl.ds(c * lanes, lanes)],
                    preferred_element_type=jnp.float32,
                ) + jnp.dot(
                    far_hot[pl.ds(r * block, block), :],
                    far_rows[:, pl.ds(c * lanes, lanes)],
                    preferred_element_type=jnp.float32,
                )
                grad[pl.ds(r * block, block), pl.ds(c * lanes, lanes)] = part
                if EDGE <= r * block < rows_dev - EDGE:
                    total = total + jnp.sum(part * part, axis=0, keepdims=True)
        fold = total[:, :128]
        for k in range(1, lanes // 128):
            fold = fold + total[:, k * 128 : (k + 1) * 128]
        squares[...] = fold
        table_copy.wait()

    return pl.pallas_call(
        kernel,
        out_shape=[
            pltpu.VMEM((rows_dev, half), jnp.float32),
            pltpu.VMEM((rows_dev, half), embed_table.dtype),
            pltpu.VMEM((1, 128), jnp.float32),
        ],
        in_specs=[any_spec(), vmem_spec(), vmem_spec(), vmem_spec(), any_spec()],
        out_specs=[vmem_spec()] * 3,
        scratch_shapes=[
            pltpu.VMEM((tokens, half), grad_rows.dtype),
            pltpu.VMEM((rows_dev, tokens), jnp.bfloat16),
            pltpu.VMEM((rows_dev, tokens), jnp.bfloat16),
            pltpu.SemaphoreType.DMA((half // lanes + 1,)),
        ],
        compiler_params=pltpu.CompilerParams(vmem_limit_bytes=18 * MIB),
        cost_estimate=pl.CostEstimate(
            flops=4 * rows_dev * tokens * half, bytes_accessed=8 * MIB, transcendentals=0
        ),
        name="local_gradient",
    )(in_hbm(grad_rows), in_vmem(swapped_rows), own_ids, swapped_ids, in_hbm(embed_table))


def edge_gradient(grad, squares, pieces, x_ids, y_ids, devices, vocab_rows):
    rows_dev, half = grad.shape
    lanes = 512

    def kernel(grad_in, squares_in, x_same, x_cross, y_same, y_cross, xi, yi, grad_out, spread, hot):
        vocab, _ = own_index()
        odd = vocab % 2
        top = rows_dev - EDGE
        start = vocab * rows_dev
        total = jnp.zeros((1, lanes), jnp.float32)
        for side, base, same, cross, ids in (
            (0, (1 - odd) * top, x_same, x_cross, xi),
            (1, odd * top, y_same, y_cross, yi),
        ):
            base = pl.multiple_of(base, EDGE)
            at = lax.broadcasted_iota(jnp.int32, (EDGE, TOK_EDGE), 0) + base
            for k in range(2):
                local = jnp.bitwise_and(ids[pl.ds(k, 1), :] - start, vocab_rows - 1)
                hot[2 * side + k] = jnp.where(at == local, 1.0, 0.0).astype(jnp.bfloat16)
            for c in range(half // lanes):
                columns = pl.ds(c * lanes, lanes)
                part = (
                    grad_in[pl.ds(base, EDGE), columns]
                    + jnp.dot(hot[2 * side], same[:, columns], preferred_element_type=jnp.float32)
                    + jnp.dot(hot[2 * side + 1], cross[:, columns], preferred_element_type=jnp.float32)
                )
                grad_out[pl.ds(base, EDGE), columns] = part
                total = total + jnp.sum(part * part, axis=0, keepdims=True)
        fold = squares_in[...]
        for k in range(lanes // 128):
            fold = fold + total[:, k * 128 : (k + 1) * 128]
        spread[...] = jnp.broadcast_to(fold, (devices, 128))

    return pl.pallas_call(
        kernel,
        out_shape=[
            pltpu.VMEM((rows_dev, half), jnp.float32),
            pltpu.VMEM((devices, 128), jnp.float32),
        ],
        in_specs=[vmem_spec()] * 8,
        out_specs=[vmem_spec()] * 2,
        scratch_shapes=[pltpu.VMEM((4, EDGE, TOK_EDGE), jnp.bfloat16)],
        input_output_aliases={0: 0},
        compiler_params=pltpu.CompilerParams(vmem_limit_bytes=4 * MIB),
        cost_estimate=pl.CostEstimate(flops=8 * EDGE * TOK_EDGE * half, bytes_accessed=4 * MIB, transcendentals=0),
        name="edge_gradient",
    )(in_vmem(grad), in_vmem(squares), *[in_vmem(piece) for piece in pieces], x_ids, y_ids)


def clipped_update(grad, own_table, partials, element_count):
    rows_dev, half = grad.shape
    devices = partials.shape[0]
    step = 128
    count = rows_dev // step

    def kernel(grad_in, table_in, sums, updated, rms, stage, sems):
        total = jnp.sum(jnp.sum(sums[...], axis=0, keepdims=True), axis=1, keepdims=True)
        grad_rms = jnp.sqrt(total / element_count)
        clip_scale = 1.0 / jnp.maximum(1.0, grad_rms / norm_limit)
        rms[0] = grad_rms[0, 0]
        rate = step_rate * clip_scale
        copies = []
        for k in range(count):
            rows = pl.ds(k * step, step)
            stage[rows, :] = (table_in[rows, :].astype(jnp.float32) - rate * grad_in[rows, :]).astype(stage.dtype)
            copy = pltpu.make_async_copy(stage.at[rows, :], updated.at[rows, :], sems.at[k])
            copy.start()
            copies.append(copy)
        for copy in copies:
            copy.wait()

    return pl.pallas_call(
        kernel,
        out_shape=[
            jax.ShapeDtypeStruct((rows_dev, half), own_table.dtype),
            jax.ShapeDtypeStruct((1,), jnp.float32),
        ],
        in_specs=[vmem_spec()] * 3,
        out_specs=[any_spec(), pl.BlockSpec(memory_space=pltpu.SMEM)],
        scratch_shapes=[
            pltpu.VMEM((rows_dev, half), own_table.dtype),
            pltpu.SemaphoreType.DMA((count,)),
        ],
        compiler_params=pltpu.CompilerParams(vmem_limit_bytes=8 * MIB),
        name="clipped_update",
    )(in_vmem(grad), in_vmem(own_table), in_vmem(partials))


def pair_routes(vocab_count, replicas, first, flip):
    routes = []
    for v in range(vocab_count):
        step = 1 if v % 2 == first else -1
        partner = (v + step) % vocab_count
        for p in range(replicas):
            routes.append((v * replicas + p, partner * replicas + (1 - p if flip else p)))
    return routes


def body(embed_table, token_ids, grad_rows):
    rows_dev, width = embed_table.shape
    vocab_count = lax.axis_size(VOCAB)
    vocab_rows = rows_dev * vocab_count
    replicas = lax.axis_size("dp")
    devices = vocab_count * replicas
    rows = grad_rows[0]
    x_near = pair_routes(vocab_count, replicas, 0, False)
    x_far = pair_routes(vocab_count, replicas, 0, True)
    y_near = pair_routes(vocab_count, replicas, 1, False)
    y_far = pair_routes(vocab_count, replicas, 1, True)
    swap = [(0, 1), (1, 0)]

    x_same, x_cross, y_same, y_cross = pack_edges(rows)
    swap_source, x_same, x_cross, y_same, y_cross = lax.optimization_barrier(
        (rows, x_same, x_cross, y_same, y_cross)
    )
    y_same = lax.ppermute(y_same, VOCAB_DP, y_near)
    x_same = lax.ppermute(x_same, VOCAB_DP, x_near)
    y_cross = lax.ppermute(y_cross, VOCAB_DP, y_far)
    x_cross = lax.ppermute(x_cross, VOCAB_DP, x_far)

    swapped_rows = lax.ppermute(pack_swap(swap_source), "dp", swap)
    swapped_ids = lax.ppermute(token_ids, "dp", swap)
    both_ids = jnp.concatenate([token_ids, swapped_ids], axis=0)
    odd = lax.axis_index("vocab_2") % 2 == 1
    first_ids, last_ids = both_ids[:, :TOK_EDGE], both_ids[:, -TOK_EDGE:]
    y_ids = lax.ppermute(jnp.where(odd, last_ids, first_ids), VOCAB_DP, y_near)
    x_ids = lax.ppermute(jnp.where(odd, first_ids, last_ids), VOCAB_DP, x_near)

    grad, own_table, squares = local_gradient(
        rows, swapped_rows, token_ids, swapped_ids, embed_table, vocab_rows
    )
    grad, spread = edge_gradient(
        grad, squares, (x_same, x_cross, y_same, y_cross), x_ids, y_ids, devices, vocab_rows
    )
    partials = lax.all_to_all(spread, VOCAB_DP, 0, 0, tiled=True)
    return tuple(clipped_update(grad, own_table, partials, vocab_rows * width))


def solution(mesh):
    split = Mesh(
        mesh.devices.reshape(4, 4, 4, mesh.shape["dp"]), ("vocab_0", "vocab_1", "vocab_2", "dp")
    )
    return jax.shard_map(
        body,
        mesh=split,
        in_specs=(P(VOCAB, None), P("dp", VOCAB), P("dp", VOCAB, None)),
        out_specs=(P(VOCAB, "dp"), P()),
        check_vma=False,
    )
```

```python
import jax
import jax.numpy as jnp
from jax import lax
from jax.experimental import pallas as pl
from jax.experimental.pallas import tpu as pltpu
from jax.sharding import Mesh
from jax.sharding import PartitionSpec as P

VOCAB = ("vocab_0", "vocab_1", "vocab_2")
VOCAB_DP = ("vocab_0", "vocab_1", "vocab_2", "dp")
TOK_EDGE = 128
EDGE = 256
LANES = 128
TAIL = 16

step_rate = 0.5
norm_limit = 1.0


MIB = 1 << 20


def own_index():
    vocab = 0
    for name in VOCAB:
        vocab = vocab * lax.axis_size(name) + lax.axis_index(name)
    return vocab, lax.axis_index("dp")


def in_vmem(value):
    return pltpu.with_memory_space_constraint(value, pltpu.VMEM)


def in_hbm(value):
    return pltpu.with_memory_space_constraint(value, pltpu.HBM)


def any_spec():
    return pl.BlockSpec(memory_space=pltpu.HBM)


def vmem_spec():
    return pl.BlockSpec(memory_space=pltpu.VMEM)


def halves(value):
    high = lax.shift_right_logical(value, 8)
    low = jnp.bitwise_and(value, 255)
    return high.astype(jnp.float32), low.astype(jnp.float32)


def joined(high, low):
    return high.astype(jnp.int32) * 256 + low.astype(jnp.int32)


def pack(grad_rows, token_ids, rows_dev, vocab_rows, edges, swap):
    tokens, width = grad_rows.shape
    half = width // 2
    tiles = half // LANES
    depth = tiles * TOK_EDGE
    parts = 8

    def kernel(rows, ids_in, *refs):
        outs, (ids, sems) = refs[:-2], refs[-2:]
        vocab, core = own_index()
        copies = [pltpu.make_async_copy(ids_in, ids, sems.at[0])]
        for out, (at, crossed) in zip(outs, edges):
            columns = pl.multiple_of((1 - core if crossed else core) * half, half)
            for c in range(tiles):
                copies.append(
                    pltpu.make_async_copy(
                        rows.at[pl.ds(at, TOK_EDGE), pl.ds(columns + c * LANES, LANES)],
                        out.at[pl.ds(c * TOK_EDGE, TOK_EDGE), :],
                        sems.at[1],
                    )
                )
        if swap:
            columns = pl.multiple_of((1 - core) * half, half)
            step = tokens // parts
            for k in range(parts):
                copies.append(
                    pltpu.make_async_copy(
                        rows.at[pl.ds(k * step, step), pl.ds(columns, half)],
                        outs[-1].at[pl.ds(k * step, step), :],
                        sems.at[1],
                    )
                )
        for copy in copies:
            copy.start()
        copies[0].wait()
        offset = jnp.bitwise_and(ids[...] - vocab * rows_dev + EDGE, vocab_rows - 1)
        for out, (at, _) in zip(outs, edges):
            high, low = halves(offset[:, at : at + TOK_EDGE])
            upper = lax.broadcasted_iota(jnp.int32, (TAIL, LANES), 0) < TAIL // 2
            out[pl.ds(depth, TAIL), :] = jnp.where(upper, high, low).astype(out.dtype)
        if swap:
            both = jnp.concatenate(halves(offset), axis=1)
            outs[-1][pl.ds(tokens, TAIL), :] = jnp.broadcast_to(both, (TAIL, half)).astype(grad_rows.dtype)
        for copy in copies[1:]:
            copy.wait()

    shapes = [pltpu.VMEM((depth + TAIL, LANES), grad_rows.dtype)] * len(edges)
    if swap:
        shapes.append(pltpu.VMEM((tokens + TAIL, half), grad_rows.dtype))
    return pl.pallas_call(
        kernel,
        out_shape=shapes,
        in_specs=[any_spec(), any_spec()],
        out_specs=[vmem_spec()] * len(shapes),
        scratch_shapes=[pltpu.VMEM((1, tokens), jnp.int32), pltpu.SemaphoreType.DMA((2,))],
        compiler_params=pltpu.CompilerParams(vmem_limit_bytes=8 * MIB),
    )(in_hbm(grad_rows), in_hbm(token_ids))


def local_gradient(grad_rows, swapped, own_ids, embed_table, vocab_rows):
    tokens, width = grad_rows.shape
    rows_dev = embed_table.shape[0]
    half = width // 2
    block = 256
    lanes = 512

    def kernel(rows, far_rows, ids, table, grad, own_table, squares, own_rows, hot, far_hot, sems):
        vocab, core = own_index()
        own = pl.multiple_of(core * half, half)
        copies = [
            pltpu.make_async_copy(
                rows.at[:, pl.ds(own + k * lanes, lanes)], own_rows.at[:, pl.ds(k * lanes, lanes)], sems.at[k]
            )
            for k in range(half // lanes)
        ]
        for copy in copies:
            copy.start()
        table_copies = [
            pltpu.make_async_copy(
                table.at[:, pl.ds(own + k * LANES, LANES)], own_table.at[k], sems.at[half // lanes]
            )
            for k in range(half // LANES)
        ]
        for copy in table_copies:
            copy.start()
        start = vocab * rows_dev
        sent = far_rows[pl.ds(tokens, TAIL), :].astype(jnp.float32)[:1, :]
        far_local = joined(sent[:, :tokens], sent[:, tokens:]) - EDGE
        own_local = jnp.bitwise_and(ids[...] - start, vocab_rows - 1)
        for one_hot, local in ((hot, own_local), (far_hot, far_local)):
            for k in range(rows_dev // block):
                at = lax.broadcasted_iota(jnp.int32, (block, tokens), 0) + k * block
                one_hot[pl.ds(k * block, block), :] = jnp.where(at == local, 1.0, 0.0).astype(jnp.bfloat16)
        total = jnp.zeros((1, lanes), jnp.float32)
        for c in range(half // lanes):
            copies[c].wait()
            for r in range(rows_dev // block):
                part = jnp.dot(
                    hot[pl.ds(r * block, block), :],
                    own_rows[:, pl.ds(c * lanes, lanes)],
                    preferred_element_type=jnp.float32,
                ) + jnp.dot(
                    far_hot[pl.ds(r * block, block), :],
                    far_rows[pl.ds(0, tokens), pl.ds(c * lanes, lanes)],
                    preferred_element_type=jnp.float32,
                )
                grad[pl.ds(r * block, block), pl.ds(c * lanes, lanes)] = part
                if EDGE <= r * block < rows_dev - EDGE:
                    total = total + jnp.sum(part * part, axis=0, keepdims=True)
        fold = total[:, :128]
        for k in range(1, lanes // 128):
            fold = fold + total[:, k * 128 : (k + 1) * 128]
        squares[...] = fold
        for copy in table_copies:
            copy.wait()

    return pl.pallas_call(
        kernel,
        out_shape=[
            pltpu.VMEM((rows_dev, half), jnp.float32),
            pltpu.VMEM((half // LANES, rows_dev, LANES), embed_table.dtype),
            pltpu.VMEM((1, 128), jnp.float32),
        ],
        in_specs=[any_spec(), vmem_spec(), vmem_spec(), any_spec()],
        out_specs=[vmem_spec()] * 3,
        scratch_shapes=[
            pltpu.VMEM((tokens, half), grad_rows.dtype),
            pltpu.VMEM((rows_dev, tokens), jnp.bfloat16),
            pltpu.VMEM((rows_dev, tokens), jnp.bfloat16),
            pltpu.SemaphoreType.DMA((half // lanes + 1,)),
        ],
        compiler_params=pltpu.CompilerParams(vmem_limit_bytes=18 * MIB),
        cost_estimate=pl.CostEstimate(
            flops=4 * rows_dev * tokens * half, bytes_accessed=8 * MIB, transcendentals=0
        ),
        name="local_gradient",
    )(in_hbm(grad_rows), in_vmem(swapped), own_ids, in_hbm(embed_table))


def edge_gradient(grad, squares, same, cross, side, spread_rows):
    rows_dev, half = grad.shape
    group = 4
    lanes = group * LANES
    depth = half // LANES * TOK_EDGE
    base = rows_dev - EDGE if side < 0 else 0
    first = 0 if side < 0 else rows_dev + EDGE

    def kernel(grad_in, squares_in, same, cross, grad_out, spread):
        total = jnp.zeros((8, lanes), jnp.float32)
        at = lax.broadcasted_iota(jnp.int32, (EDGE, TOK_EDGE), 0) + first
        hot = []
        for part in (same, cross):
            sent = part[pl.ds(depth, TAIL), :].astype(jnp.float32)
            offset = joined(sent[:1, :], sent[TAIL // 2 : TAIL // 2 + 1, :])
            hot.append(jnp.where(at == offset, 1.0, 0.0).astype(jnp.bfloat16))
        hot = jnp.concatenate(hot, axis=1)
        for c in range(half // lanes):
            columns = pl.ds(c * lanes, lanes)
            rows = jnp.concatenate(
                [
                    jnp.concatenate(
                        [part[pl.ds((c * group + g) * TOK_EDGE, TOK_EDGE), :] for g in range(group)], axis=1
                    )
                    for part in (same, cross)
                ],
                axis=0,
            )
            value = grad_in[pl.ds(base, EDGE), columns] + jnp.dot(
                hot, rows, preferred_element_type=jnp.float32
            )
            grad_out[pl.ds(base, EDGE), columns] = value
            total = total + jnp.sum((value * value).reshape(EDGE // 8, 8, lanes), axis=0)
        total = jnp.sum(total, axis=0, keepdims=True)
        fold = squares_in[...]
        for k in range(group):
            fold = fold + total[:, k * LANES : (k + 1) * LANES]
        spread[...] = jnp.broadcast_to(fold, (spread_rows, LANES))

    return pl.pallas_call(
        kernel,
        out_shape=[
            pltpu.VMEM((rows_dev, half), jnp.float32),
            pltpu.VMEM((spread_rows, LANES), jnp.float32),
        ],
        in_specs=[vmem_spec()] * 4,
        out_specs=[vmem_spec()] * 2,
        input_output_aliases={0: 0},
        compiler_params=pltpu.CompilerParams(vmem_limit_bytes=4 * MIB),
        cost_estimate=pl.CostEstimate(flops=4 * EDGE * TOK_EDGE * half, bytes_accessed=2 * MIB, transcendentals=0),
    )(in_vmem(grad), in_vmem(squares), in_vmem(same), in_vmem(cross))


def clipped_update(grad, own_table, partials, element_count):
    rows_dev, half = grad.shape
    tiles = half // LANES
    step = 64

    def kernel(grad_in, table_in, sums, updated, rms_out, stage, rms, sems):
        total = jnp.sum(jnp.sum(sums[...], axis=0, keepdims=True), axis=1, keepdims=True)
        grad_rms = jnp.sqrt(total / element_count)
        clip_scale = 1.0 / jnp.maximum(1.0, grad_rms / norm_limit)
        rate = step_rate * clip_scale
        rms[0] = grad_rms[0, 0]
        copies = [pltpu.make_async_copy(rms, rms_out, sems.at[tiles])]
        copies[0].start()
        for c in range(tiles):
            columns = pl.ds(c * LANES, LANES)
            for r in range(0, rows_dev, step):
                rows = pl.ds(r, step)
                stage[c, rows, :] = (
                    table_in[c, rows, :].astype(jnp.float32) - rate * grad_in[rows, columns]
                ).astype(stage.dtype)
            copies.append(pltpu.make_async_copy(stage.at[c], updated.at[:, columns], sems.at[c]))
            copies[-1].start()
        for copy in copies:
            copy.wait()

    return pl.pallas_call(
        kernel,
        out_shape=[
            jax.ShapeDtypeStruct((rows_dev, half), own_table.dtype),
            jax.ShapeDtypeStruct((1,), jnp.float32),
        ],
        in_specs=[vmem_spec()] * 3,
        out_specs=[any_spec(), any_spec()],
        scratch_shapes=[
            pltpu.VMEM((tiles, rows_dev, LANES), own_table.dtype),
            pltpu.SMEM((1,), jnp.float32),
            pltpu.SemaphoreType.DMA((tiles + 1,)),
        ],
        compiler_params=pltpu.CompilerParams(vmem_limit_bytes=8 * MIB),
        name="clipped_update",
    )(in_vmem(grad), in_vmem(own_table), in_vmem(partials))


def routes(vocab_count, replicas, step, flip):
    return [
        (v * replicas + p, (v + step) % vocab_count * replicas + (1 - p if flip else p))
        for v in range(vocab_count)
        for p in range(replicas)
    ]


def body(embed_table, token_ids, grad_rows):
    rows_dev, width = embed_table.shape
    vocab_count = lax.axis_size(VOCAB)
    vocab_rows = rows_dev * vocab_count
    replicas = lax.axis_size("dp")
    devices = vocab_count * replicas
    rows = grad_rows[0]

    def sent(piece, step, flip):
        return lax.ppermute(piece, VOCAB_DP, routes(vocab_count, replicas, step, flip))

    last = token_ids.shape[1] - TOK_EDGE
    shape = (rows_dev, vocab_rows)
    plus_same, minus_same = pack(rows, token_ids, *shape, ((last, False), (0, False)), False)
    plus_same = sent(plus_same, 1, False)
    minus_same = sent(minus_same, -1, False)
    plus_cross, minus_cross, far = pack(rows, token_ids, *shape, ((last, True), (0, True)), True)
    far = sent(far, 0, True)
    plus_cross = sent(plus_cross, 1, True)
    minus_cross = sent(minus_cross, -1, True)
    grad, own_table, squares = local_gradient(rows, far, token_ids, embed_table, vocab_rows)
    grad, squares = edge_gradient(grad, squares, plus_same, plus_cross, 1, 1)
    grad, spread = edge_gradient(grad, squares, minus_same, minus_cross, -1, devices)
    partials = lax.all_to_all(spread, VOCAB_DP, 0, 0, tiled=True)
    return tuple(clipped_update(grad, own_table, partials, vocab_rows * width))


def solution(mesh):
    split = Mesh(
        mesh.devices.reshape(4, 4, 4, mesh.shape["dp"]), ("vocab_0", "vocab_1", "vocab_2", "dp")
    )
    return jax.shard_map(
        body,
        mesh=split,
        in_specs=(P(VOCAB, None), P("dp", VOCAB), P("dp", VOCAB, None)),
        out_specs=(P(VOCAB, "dp"), P()),
        check_vma=False,
    )
```

```python
import jax
import jax.numpy as jnp
from jax import lax
from jax.experimental import pallas as pl
from jax.experimental.pallas import tpu as pltpu
from jax.sharding import Mesh
from jax.sharding import PartitionSpec as P

VOCAB = ("vocab_0", "vocab_1", "vocab_2")
VOCAB_DP = ("vocab_0", "vocab_1", "vocab_2", "dp")
TOK_EDGE = 128
EDGE = 256
LANES = 128
TAIL = 16

step_rate = 0.5
norm_limit = 1.0


MIB = 1 << 20


def own_index():
    vocab = 0
    for name in VOCAB:
        vocab = vocab * lax.axis_size(name) + lax.axis_index(name)
    return vocab, lax.axis_index("dp")


def in_vmem(value):
    return pltpu.with_memory_space_constraint(value, pltpu.VMEM)


def in_hbm(value):
    return pltpu.with_memory_space_constraint(value, pltpu.HBM)


def any_spec():
    return pl.BlockSpec(memory_space=pltpu.HBM)


def vmem_spec():
    return pl.BlockSpec(memory_space=pltpu.VMEM)


def halves(value):
    high = lax.shift_right_logical(value, 8)
    low = jnp.bitwise_and(value, 255)
    return high.astype(jnp.float32), low.astype(jnp.float32)


def joined(high, low):
    return high.astype(jnp.int32) * 256 + low.astype(jnp.int32)


def pack(grad_rows, token_ids, rows_dev, vocab_rows, edges, swap):
    tokens, width = grad_rows.shape
    half = width // 2
    parts = 8

    def kernel(rows, ids_in, *refs):
        outs, (ids, sems) = refs[:-2], refs[-2:]
        vocab, core = own_index()
        copies = [pltpu.make_async_copy(ids_in, ids, sems.at[0])]
        for out, (at, crossed, first, count, _) in zip(outs, edges):
            columns = pl.multiple_of((1 - core if crossed else core) * half, half)
            for c in range(count):
                copies.append(
                    pltpu.make_async_copy(
                        rows.at[pl.ds(at, TOK_EDGE), pl.ds(columns + (first + c) * LANES, LANES)],
                        out.at[pl.ds(c * TOK_EDGE, TOK_EDGE), :],
                        sems.at[1],
                    )
                )
        if swap:
            columns = pl.multiple_of((1 - core) * half, half)
            step = tokens // parts
            for k in range(parts):
                copies.append(
                    pltpu.make_async_copy(
                        rows.at[pl.ds(k * step, step), pl.ds(columns, half)],
                        outs[-1].at[pl.ds(k * step, step), :],
                        sems.at[1],
                    )
                )
        for copy in copies:
            copy.start()
        copies[0].wait()
        offset = jnp.bitwise_and(ids[...] - vocab * rows_dev + EDGE, vocab_rows - 1)
        for out, (at, _, _, count, tail) in zip(outs, edges):
            if tail:
                high, low = halves(offset[:, at : at + TOK_EDGE])
                upper = lax.broadcasted_iota(jnp.int32, (TAIL, LANES), 0) < TAIL // 2
                out[pl.ds(count * TOK_EDGE, TAIL), :] = jnp.where(upper, high, low).astype(out.dtype)
        if swap:
            both = jnp.concatenate(halves(offset), axis=1)
            outs[-1][pl.ds(tokens, TAIL), :] = jnp.broadcast_to(both, (TAIL, half)).astype(grad_rows.dtype)
        for copy in copies[1:]:
            copy.wait()

    shapes = [
        pltpu.VMEM((count * TOK_EDGE + (TAIL if tail else 0), LANES), grad_rows.dtype)
        for _, _, _, count, tail in edges
    ]
    if swap:
        shapes.append(pltpu.VMEM((tokens + TAIL, half), grad_rows.dtype))
    return pl.pallas_call(
        kernel,
        out_shape=shapes,
        in_specs=[any_spec(), any_spec()],
        out_specs=[vmem_spec()] * len(shapes),
        scratch_shapes=[pltpu.VMEM((1, tokens), jnp.int32), pltpu.SemaphoreType.DMA((2,))],
        compiler_params=pltpu.CompilerParams(vmem_limit_bytes=8 * MIB),
    )(in_hbm(grad_rows), in_hbm(token_ids))


def local_gradient(grad_rows, swapped, own_ids, embed_table, vocab_rows):
    tokens, width = grad_rows.shape
    rows_dev = embed_table.shape[0]
    half = width // 2
    block = 256
    lanes = 512

    def kernel(rows, far_rows, ids, table, grad, own_table, squares, own_rows, hot, far_hot, sems):
        vocab, core = own_index()
        own = pl.multiple_of(core * half, half)
        copies = [
            pltpu.make_async_copy(
                rows.at[:, pl.ds(own + k * lanes, lanes)], own_rows.at[:, pl.ds(k * lanes, lanes)], sems.at[k]
            )
            for k in range(half // lanes)
        ]
        for copy in copies:
            copy.start()
        table_copies = [
            pltpu.make_async_copy(
                table.at[:, pl.ds(own + k * LANES, LANES)], own_table.at[k], sems.at[half // lanes]
            )
            for k in range(half // LANES)
        ]
        for copy in table_copies:
            copy.start()
        start = vocab * rows_dev
        sent = far_rows[pl.ds(tokens, TAIL), :].astype(jnp.float32)[:1, :]
        far_local = joined(sent[:, :tokens], sent[:, tokens:]) - EDGE
        own_local = jnp.bitwise_and(ids[...] - start, vocab_rows - 1)
        for one_hot, local in ((hot, own_local), (far_hot, far_local)):
            for k in range(rows_dev // block):
                at = lax.broadcasted_iota(jnp.int32, (block, tokens), 0) + k * block
                one_hot[pl.ds(k * block, block), :] = jnp.where(at == local, 1.0, 0.0).astype(jnp.bfloat16)
        total = jnp.zeros((1, lanes), jnp.float32)
        for c in range(half // lanes):
            copies[c].wait()
            for r in range(rows_dev // block):
                part = jnp.dot(
                    hot[pl.ds(r * block, block), :],
                    own_rows[:, pl.ds(c * lanes, lanes)],
                    preferred_element_type=jnp.float32,
                ) + jnp.dot(
                    far_hot[pl.ds(r * block, block), :],
                    far_rows[pl.ds(0, tokens), pl.ds(c * lanes, lanes)],
                    preferred_element_type=jnp.float32,
                )
                grad[pl.ds(r * block, block), pl.ds(c * lanes, lanes)] = part
                if EDGE <= r * block < rows_dev - EDGE:
                    total = total + jnp.sum(part * part, axis=0, keepdims=True)
        fold = total[:, :128]
        for k in range(1, lanes // 128):
            fold = fold + total[:, k * 128 : (k + 1) * 128]
        squares[...] = fold
        for copy in table_copies:
            copy.wait()

    return pl.pallas_call(
        kernel,
        out_shape=[
            pltpu.VMEM((rows_dev, half), jnp.float32),
            pltpu.VMEM((half // LANES, rows_dev, LANES), embed_table.dtype),
            pltpu.VMEM((1, 128), jnp.float32),
        ],
        in_specs=[any_spec(), vmem_spec(), vmem_spec(), any_spec()],
        out_specs=[vmem_spec()] * 3,
        scratch_shapes=[
            pltpu.VMEM((tokens, half), grad_rows.dtype),
            pltpu.VMEM((rows_dev, tokens), jnp.bfloat16),
            pltpu.VMEM((rows_dev, tokens), jnp.bfloat16),
            pltpu.SemaphoreType.DMA((half // lanes + 1,)),
        ],
        compiler_params=pltpu.CompilerParams(vmem_limit_bytes=18 * MIB),
        cost_estimate=pl.CostEstimate(
            flops=4 * rows_dev * tokens * half, bytes_accessed=8 * MIB, transcendentals=0
        ),
        name="local_gradient",
    )(in_hbm(grad_rows), in_vmem(swapped), own_ids, in_hbm(embed_table))


def edge_gradient(grad, squares, same, cross, rest, side, spread_rows):
    rows_dev, half = grad.shape
    group = 4
    lanes = group * LANES
    base = rows_dev - EDGE if side < 0 else 0
    first = 0 if side < 0 else rows_dev + EDGE

    def kernel(grad_in, squares_in, same, cross, *refs):
        others, (grad_out, spread) = refs[:-2], refs[-2:]

        def tile(part, k):
            whole = part.shape[0] // TOK_EDGE
            if k < whole:
                return part[pl.ds(k * TOK_EDGE, TOK_EDGE), :]
            rows = pl.ds((k - whole) * TOK_EDGE, TOK_EDGE)
            return others[0][rows, :] + others[1][rows, :]

        total = jnp.zeros((8, lanes), jnp.float32)
        at = lax.broadcasted_iota(jnp.int32, (EDGE, TOK_EDGE), 0) + first
        hot = []
        for part in (same, cross):
            sent = part[pl.ds(part.shape[0] - TAIL, TAIL), :].astype(jnp.float32)
            offset = joined(sent[:1, :], sent[TAIL // 2 : TAIL // 2 + 1, :])
            hot.append(jnp.where(at == offset, 1.0, 0.0).astype(jnp.bfloat16))
        hot = jnp.concatenate(hot, axis=1)
        for c in range(half // lanes):
            columns = pl.ds(c * lanes, lanes)
            rows = jnp.concatenate(
                [
                    jnp.concatenate(
                        [tile(part, c * group + g) for g in range(group)], axis=1
                    )
                    for part in (same, cross)
                ],
                axis=0,
            )
            value = grad_in[pl.ds(base, EDGE), columns] + jnp.dot(
                hot, rows, preferred_element_type=jnp.float32
            )
            grad_out[pl.ds(base, EDGE), columns] = value
            total = total + jnp.sum((value * value).reshape(EDGE // 8, 8, lanes), axis=0)
        total = jnp.sum(total, axis=0, keepdims=True)
        fold = squares_in[...]
        for k in range(group):
            fold = fold + total[:, k * LANES : (k + 1) * LANES]
        spread[...] = jnp.broadcast_to(fold, (spread_rows, LANES))

    return pl.pallas_call(
        kernel,
        out_shape=[
            pltpu.VMEM((rows_dev, half), jnp.float32),
            pltpu.VMEM((spread_rows, LANES), jnp.float32),
        ],
        in_specs=[vmem_spec()] * (4 + len(rest)),
        out_specs=[vmem_spec()] * 2,
        input_output_aliases={0: 0},
        compiler_params=pltpu.CompilerParams(vmem_limit_bytes=4 * MIB),
        cost_estimate=pl.CostEstimate(flops=4 * EDGE * TOK_EDGE * half, bytes_accessed=2 * MIB, transcendentals=0),
    )(in_vmem(grad), in_vmem(squares), in_vmem(same), in_vmem(cross), *[in_vmem(part) for part in rest])


def clipped_update(grad, own_table, partials, element_count):
    rows_dev, half = grad.shape
    tiles = half // LANES
    step = 64

    def kernel(grad_in, table_in, sums, updated, rms_out, stage, rms, sems):
        total = jnp.sum(jnp.sum(sums[...], axis=0, keepdims=True), axis=1, keepdims=True)
        grad_rms = jnp.sqrt(total / element_count)
        clip_scale = 1.0 / jnp.maximum(1.0, grad_rms / norm_limit)
        rate = step_rate * clip_scale
        rms[0] = grad_rms[0, 0]
        copies = [pltpu.make_async_copy(rms, rms_out, sems.at[tiles])]
        copies[0].start()
        for c in range(tiles):
            columns = pl.ds(c * LANES, LANES)
            for r in range(0, rows_dev, step):
                rows = pl.ds(r, step)
                stage[c, rows, :] = (
                    table_in[c, rows, :].astype(jnp.float32) - rate * grad_in[rows, columns]
                ).astype(stage.dtype)
            copies.append(pltpu.make_async_copy(stage.at[c], updated.at[:, columns], sems.at[c]))
            copies[-1].start()
        for copy in copies:
            copy.wait()

    return pl.pallas_call(
        kernel,
        out_shape=[
            jax.ShapeDtypeStruct((rows_dev, half), own_table.dtype),
            jax.ShapeDtypeStruct((1,), jnp.float32),
        ],
        in_specs=[vmem_spec()] * 3,
        out_specs=[any_spec(), any_spec()],
        scratch_shapes=[
            pltpu.VMEM((tiles, rows_dev, LANES), own_table.dtype),
            pltpu.SMEM((1,), jnp.float32),
            pltpu.SemaphoreType.DMA((tiles + 1,)),
        ],
        compiler_params=pltpu.CompilerParams(vmem_limit_bytes=8 * MIB),
        name="clipped_update",
    )(in_vmem(grad), in_vmem(own_table), in_vmem(partials))


def routes(vocab_count, replicas, step, flip, left_out=()):
    return [
        (v * replicas + p, (v + step) % vocab_count * replicas + (1 - p if flip else p))
        for v in range(vocab_count)
        for p in range(replicas)
        if v not in left_out
    ]


def body(embed_table, token_ids, grad_rows):
    rows_dev, width = embed_table.shape
    vocab_count = lax.axis_size(VOCAB)
    vocab_rows = rows_dev * vocab_count
    replicas = lax.axis_size("dp")
    devices = vocab_count * replicas
    rows = grad_rows[0]
    plane = vocab_count // lax.axis_size(VOCAB[0])
    line = lax.axis_size(VOCAB[2])
    corners = range(0, vocab_count, plane)
    relays = {v: v + 2 * line - 1 for v in corners}
    to_relay = [(v * replicas + p, relays[v] * replicas + 1 - p) for v in corners for p in range(replicas)]
    from_relay = [
        (relays[v] * replicas + p, (v - 1) % vocab_count * replicas + p) for v in corners for p in range(replicas)
    ]

    def moved(piece, pairs):
        return lax.ppermute(piece, VOCAB_DP, pairs)

    def sent(piece, step, flip, left_out=()):
        return moved(piece, routes(vocab_count, replicas, step, flip, left_out))

    last = token_ids.shape[1] - TOK_EDGE
    tiles = width // replicas // LANES
    kept = tiles - tiles // 4
    shape = (rows_dev, vocab_rows)
    plus_same, minus_same, minus_rest = pack(
        rows,
        token_ids,
        *shape,
        (
            (last, False, 0, tiles, True),
            (0, False, 0, tiles, True),
            (0, True, kept, tiles - kept, False),
        ),
        False,
    )
    plus_same = sent(plus_same, 1, False)
    minus_same = sent(minus_same, -1, False)
    relayed = moved(minus_rest, to_relay)
    plus_cross, minus_cross, far = pack(
        rows, token_ids, *shape, ((last, True, 0, tiles, True), (0, True, 0, kept, True)), True
    )
    far = sent(far, 0, True)
    minus_cross = sent(minus_cross, -1, True)
    plus_cross = sent(plus_cross, 1, True)
    minus_rest = sent(minus_rest, -1, True, corners)
    relayed = moved(relayed, from_relay)
    grad, own_table, squares = local_gradient(rows, far, token_ids, embed_table, vocab_rows)
    grad, squares = edge_gradient(grad, squares, plus_same, plus_cross, (), 1, 1)
    grad, spread = edge_gradient(grad, squares, minus_same, minus_cross, (minus_rest, relayed), -1, devices)
    partials = lax.all_to_all(spread, VOCAB_DP, 0, 0, tiled=True)
    return tuple(clipped_update(grad, own_table, partials, vocab_rows * width))


def solution(mesh):
    split = Mesh(
        mesh.devices.reshape(4, 4, 4, mesh.shape["dp"]), ("vocab_0", "vocab_1", "vocab_2", "dp")
    )
    return jax.shard_map(
        body,
        mesh=split,
        in_specs=(P(VOCAB, None), P("dp", VOCAB), P("dp", VOCAB, None)),
        out_specs=(P(VOCAB, "dp"), P()),
        check_vma=False,
    )
```

```python
import jax
import jax.numpy as jnp
from jax import lax
from jax.experimental import pallas as pl
from jax.experimental.pallas import tpu as pltpu
from jax.sharding import Mesh
from jax.sharding import PartitionSpec as P

VOCAB = ("vocab_0", "vocab_1", "vocab_2")
VOCAB_DP = ("vocab_0", "vocab_1", "vocab_2", "dp")
TOK_EDGE = 128
EDGE = 256
LANES = 128
TAIL = 16

step_rate = 0.5
norm_limit = 1.0


MIB = 1 << 20


def own_index():
    vocab = 0
    for name in VOCAB:
        vocab = vocab * lax.axis_size(name) + lax.axis_index(name)
    return vocab, lax.axis_index("dp")


def in_vmem(value):
    return pltpu.with_memory_space_constraint(value, pltpu.VMEM)


def in_hbm(value):
    return pltpu.with_memory_space_constraint(value, pltpu.HBM)


def any_spec():
    return pl.BlockSpec(memory_space=pltpu.HBM)


def vmem_spec():
    return pl.BlockSpec(memory_space=pltpu.VMEM)


def halves(value):
    high = lax.shift_right_logical(value, 8)
    low = jnp.bitwise_and(value, 255)
    return high.astype(jnp.float32), low.astype(jnp.float32)


def joined(high, low):
    return high.astype(jnp.int32) * 256 + low.astype(jnp.int32)


def pack(grad_rows, token_ids, rows_dev, vocab_rows, edges, swap):
    tokens, width = grad_rows.shape
    half = width // 2
    parts = 8

    def kernel(rows, ids_in, *refs):
        outs, (ids, sems) = refs[:-2], refs[-2:]
        vocab, core = own_index()
        copies = [pltpu.make_async_copy(ids_in, ids, sems.at[0])]
        for out, (at, crossed, first, count, _) in zip(outs, edges):
            columns = pl.multiple_of((1 - core if crossed else core) * half, half)
            for c in range(count):
                copies.append(
                    pltpu.make_async_copy(
                        rows.at[pl.ds(at, TOK_EDGE), pl.ds(columns + (first + c) * LANES, LANES)],
                        out.at[pl.ds(c * TOK_EDGE, TOK_EDGE), :],
                        sems.at[1],
                    )
                )
        if swap:
            columns = pl.multiple_of((1 - core) * half, half)
            step = tokens // parts
            for k in range(parts):
                copies.append(
                    pltpu.make_async_copy(
                        rows.at[pl.ds(k * step, step), pl.ds(columns, half)],
                        outs[-1].at[pl.ds(k * step, step), :],
                        sems.at[1],
                    )
                )
        for copy in copies:
            copy.start()
        copies[0].wait()
        offset = jnp.bitwise_and(ids[...] - vocab * rows_dev + EDGE, vocab_rows - 1)
        for out, (at, _, _, count, tail) in zip(outs, edges):
            if tail:
                high, low = halves(offset[:, at : at + TOK_EDGE])
                upper = lax.broadcasted_iota(jnp.int32, (TAIL, LANES), 0) < TAIL // 2
                out[pl.ds(count * TOK_EDGE, TAIL), :] = jnp.where(upper, high, low).astype(out.dtype)
        if swap:
            both = jnp.concatenate(halves(offset), axis=1)
            outs[-1][pl.ds(tokens, TAIL), :] = jnp.broadcast_to(both, (TAIL, half)).astype(grad_rows.dtype)
        for copy in copies[1:]:
            copy.wait()

    shapes = [
        pltpu.VMEM((count * TOK_EDGE + (TAIL if tail else 0), LANES), grad_rows.dtype)
        for _, _, _, count, tail in edges
    ]
    if swap:
        shapes.append(pltpu.VMEM((tokens + TAIL, half), grad_rows.dtype))
    return pl.pallas_call(
        kernel,
        out_shape=shapes,
        in_specs=[any_spec(), any_spec()],
        out_specs=[vmem_spec()] * len(shapes),
        scratch_shapes=[pltpu.VMEM((1, tokens), jnp.int32), pltpu.SemaphoreType.DMA((2,))],
        compiler_params=pltpu.CompilerParams(vmem_limit_bytes=8 * MIB),
    )(in_hbm(grad_rows), in_hbm(token_ids))


def local_gradient(grad_rows, swapped, own_ids, embed_table, vocab_rows):
    tokens, width = grad_rows.shape
    rows_dev = embed_table.shape[0]
    half = width // 2
    block = 256
    lanes = 512
    token_blocks = tokens // block
    row_blocks = rows_dev // block

    def kernel(rows, far_rows, ids_in, table, grad, own_table, squares, own_rows, ids, sems):
        vocab, core = own_index()
        own = pl.multiple_of(core * half, half)
        copies = [
            pltpu.make_async_copy(
                rows.at[pl.ds(k * block, block), pl.ds(own, half)], own_rows.at[pl.ds(k * block, block), :], sems.at[k]
            )
            for k in range(token_blocks)
        ]
        table_copies = [
            pltpu.make_async_copy(
                table.at[:, pl.ds(own + k * LANES, LANES)], own_table.at[k], sems.at[token_blocks]
            )
            for k in range(half // LANES)
        ]
        ids_copy = pltpu.make_async_copy(ids_in, ids, sems.at[token_blocks + 1])
        for copy in [ids_copy] + copies + table_copies:
            copy.start()
        for k in range(rows_dev // 64):
            grad[pl.ds(k * 64, 64), :] = jnp.zeros((64, half), jnp.float32)

        def accumulate(local, token_rows, ready):
            firsts = [local[0, k * block] for k in range(token_blocks)]
            for k in range(token_blocks):
                part = local[:, k * block : (k + 1) * block]
                low = jnp.maximum(lax.shift_right_arithmetic(firsts[k], 8), 0)
                high = row_blocks - 1
                if k + 1 < token_blocks:
                    high = jnp.minimum(lax.shift_right_arithmetic(firsts[k + 1], 8), high)
                ready(k)

                def step(r, carry):
                    base = pl.multiple_of(r * block, block)
                    at = lax.broadcasted_iota(jnp.int32, (block, block), 0) + base
                    hot = jnp.where(at == part, 1.0, 0.0).astype(jnp.bfloat16)
                    for c in range(half // lanes):
                        columns = pl.ds(c * lanes, lanes)
                        grad[pl.ds(base, block), columns] += jnp.dot(
                            hot, token_rows[pl.ds(k * block, block), columns], preferred_element_type=jnp.float32
                        )
                    return carry

                lax.fori_loop(low, high + 1, step, 0)

        sent = far_rows[pl.ds(tokens, TAIL), :].astype(jnp.float32)[:1, :]
        accumulate(joined(sent[:, :tokens], sent[:, tokens:]) - EDGE, far_rows, lambda k: None)
        ids_copy.wait()
        offset = jnp.bitwise_and(ids[...] - vocab * rows_dev + EDGE, vocab_rows - 1)
        accumulate(offset - EDGE, own_rows, lambda k: copies[k].wait())
        total = jnp.zeros((8, lanes), jnp.float32)
        for r in range(EDGE, rows_dev - EDGE, 64):
            for c in range(half // lanes):
                value = grad[pl.ds(r, 64), pl.ds(c * lanes, lanes)]
                total = total + jnp.sum((value * value).reshape(8, 8, lanes), axis=0)
        total = jnp.sum(total, axis=0, keepdims=True)
        fold = total[:, :LANES]
        for k in range(1, lanes // LANES):
            fold = fold + total[:, k * LANES : (k + 1) * LANES]
        squares[...] = fold
        for copy in table_copies:
            copy.wait()

    return pl.pallas_call(
        kernel,
        out_shape=[
            pltpu.VMEM((rows_dev, half), jnp.float32),
            pltpu.VMEM((half // LANES, rows_dev, LANES), embed_table.dtype),
            pltpu.VMEM((1, LANES), jnp.float32),
        ],
        in_specs=[any_spec(), vmem_spec(), any_spec(), any_spec()],
        out_specs=[vmem_spec()] * 3,
        scratch_shapes=[
            pltpu.VMEM((tokens, half), grad_rows.dtype),
            pltpu.VMEM((1, tokens), jnp.int32),
            pltpu.SemaphoreType.DMA((token_blocks + 2,)),
        ],
        compiler_params=pltpu.CompilerParams(vmem_limit_bytes=12 * MIB),
        cost_estimate=pl.CostEstimate(
            flops=4 * rows_dev * tokens * half, bytes_accessed=8 * MIB, transcendentals=0
        ),
        name="local_gradient",
    )(in_hbm(grad_rows), in_vmem(swapped), in_hbm(own_ids), in_hbm(embed_table))


def edge_gradient(grad, squares, same, cross, rest, side, spread_rows):
    rows_dev, half = grad.shape
    group = 4
    lanes = group * LANES
    base = rows_dev - EDGE if side < 0 else 0
    first = 0 if side < 0 else rows_dev + EDGE

    def kernel(grad_in, squares_in, same, cross, *refs):
        others, (grad_out, spread) = refs[:-2], refs[-2:]

        def tile(part, k):
            whole = part.shape[0] // TOK_EDGE
            if k < whole:
                return part[pl.ds(k * TOK_EDGE, TOK_EDGE), :]
            rows = pl.ds((k - whole) * TOK_EDGE, TOK_EDGE)
            return others[0][rows, :] + others[1][rows, :]

        total = jnp.zeros((8, lanes), jnp.float32)
        at = lax.broadcasted_iota(jnp.int32, (EDGE, TOK_EDGE), 0) + first
        hot = []
        for part in (same, cross):
            sent = part[pl.ds(part.shape[0] - TAIL, TAIL), :].astype(jnp.float32)
            offset = joined(sent[:1, :], sent[TAIL // 2 : TAIL // 2 + 1, :])
            hot.append(jnp.where(at == offset, 1.0, 0.0).astype(jnp.bfloat16))
        hot = jnp.concatenate(hot, axis=1)
        for c in range(half // lanes):
            columns = pl.ds(c * lanes, lanes)
            rows = jnp.concatenate(
                [
                    jnp.concatenate(
                        [tile(part, c * group + g) for g in range(group)], axis=1
                    )
                    for part in (same, cross)
                ],
                axis=0,
            )
            value = grad_in[pl.ds(base, EDGE), columns] + jnp.dot(
                hot, rows, preferred_element_type=jnp.float32
            )
            grad_out[pl.ds(base, EDGE), columns] = value
            total = total + jnp.sum((value * value).reshape(EDGE // 8, 8, lanes), axis=0)
        total = jnp.sum(total, axis=0, keepdims=True)
        fold = squares_in[...]
        for k in range(group):
            fold = fold + total[:, k * LANES : (k + 1) * LANES]
        spread[...] = jnp.broadcast_to(fold, (spread_rows, LANES))

    return pl.pallas_call(
        kernel,
        out_shape=[
            pltpu.VMEM((rows_dev, half), jnp.float32),
            pltpu.VMEM((spread_rows, LANES), jnp.float32),
        ],
        in_specs=[vmem_spec()] * (4 + len(rest)),
        out_specs=[vmem_spec()] * 2,
        input_output_aliases={0: 0},
        compiler_params=pltpu.CompilerParams(vmem_limit_bytes=4 * MIB),
        cost_estimate=pl.CostEstimate(flops=4 * EDGE * TOK_EDGE * half, bytes_accessed=2 * MIB, transcendentals=0),
    )(in_vmem(grad), in_vmem(squares), in_vmem(same), in_vmem(cross), *[in_vmem(part) for part in rest])


def clipped_update(grad, own_table, partials, element_count):
    rows_dev, half = grad.shape
    tiles = half // LANES
    step = 64

    def kernel(grad_in, table_in, sums, updated, rms_out, stage, rms, sems):
        total = jnp.sum(jnp.sum(sums[...], axis=0, keepdims=True), axis=1, keepdims=True)
        grad_rms = jnp.sqrt(total / element_count)
        clip_scale = 1.0 / jnp.maximum(1.0, grad_rms / norm_limit)
        rate = step_rate * clip_scale
        rms[0] = grad_rms[0, 0]
        copies = [pltpu.make_async_copy(rms, rms_out, sems.at[tiles])]
        copies[0].start()
        for c in range(tiles):
            columns = pl.ds(c * LANES, LANES)
            for r in range(0, rows_dev, step):
                rows = pl.ds(r, step)
                stage[c, rows, :] = (
                    table_in[c, rows, :].astype(jnp.float32) - rate * grad_in[rows, columns]
                ).astype(stage.dtype)
            copies.append(pltpu.make_async_copy(stage.at[c], updated.at[:, columns], sems.at[c]))
            copies[-1].start()
        for copy in copies:
            copy.wait()

    return pl.pallas_call(
        kernel,
        out_shape=[
            jax.ShapeDtypeStruct((rows_dev, half), own_table.dtype),
            jax.ShapeDtypeStruct((1,), jnp.float32),
        ],
        in_specs=[vmem_spec()] * 3,
        out_specs=[any_spec(), any_spec()],
        scratch_shapes=[
            pltpu.VMEM((tiles, rows_dev, LANES), own_table.dtype),
            pltpu.SMEM((1,), jnp.float32),
            pltpu.SemaphoreType.DMA((tiles + 1,)),
        ],
        compiler_params=pltpu.CompilerParams(vmem_limit_bytes=8 * MIB),
        name="clipped_update",
    )(in_vmem(grad), in_vmem(own_table), in_vmem(partials))


def routes(vocab_count, replicas, step, flip, left_out=()):
    return [
        (v * replicas + p, (v + step) % vocab_count * replicas + (1 - p if flip else p))
        for v in range(vocab_count)
        for p in range(replicas)
        if v not in left_out
    ]


def body(embed_table, token_ids, grad_rows):
    rows_dev, width = embed_table.shape
    vocab_count = lax.axis_size(VOCAB)
    vocab_rows = rows_dev * vocab_count
    replicas = lax.axis_size("dp")
    devices = vocab_count * replicas
    rows = grad_rows[0]
    plane = vocab_count // lax.axis_size(VOCAB[0])
    line = lax.axis_size(VOCAB[2])
    corners = range(0, vocab_count, plane)
    relays = {v: v + 2 * line - 1 for v in corners}
    to_relay = [(v * replicas + p, relays[v] * replicas + 1 - p) for v in corners for p in range(replicas)]
    from_relay = [
        (relays[v] * replicas + p, (v - 1) % vocab_count * replicas + p) for v in corners for p in range(replicas)
    ]

    def moved(piece, pairs):
        return lax.ppermute(piece, VOCAB_DP, pairs)

    def sent(piece, step, flip, left_out=()):
        return moved(piece, routes(vocab_count, replicas, step, flip, left_out))

    last = token_ids.shape[1] - TOK_EDGE
    tiles = width // replicas // LANES
    kept = tiles - 3
    shape = (rows_dev, vocab_rows)
    plus_same, minus_same, minus_rest = pack(
        rows,
        token_ids,
        *shape,
        (
            (last, False, 0, tiles, True),
            (0, False, 0, tiles, True),
            (0, True, kept, tiles - kept, False),
        ),
        False,
    )
    plus_same = sent(plus_same, 1, False)
    minus_same = sent(minus_same, -1, False)
    relayed = moved(minus_rest, to_relay)
    plus_cross, minus_cross, far = pack(
        rows, token_ids, *shape, ((last, True, 0, tiles, True), (0, True, 0, kept, True)), True
    )
    far = sent(far, 0, True)
    minus_cross = sent(minus_cross, -1, True)
    plus_cross = sent(plus_cross, 1, True)
    minus_rest = sent(minus_rest, -1, True, corners)
    relayed = moved(relayed, from_relay)
    grad, own_table, squares = local_gradient(rows, far, token_ids, embed_table, vocab_rows)
    grad, squares = edge_gradient(grad, squares, plus_same, plus_cross, (), 1, 1)
    grad, spread = edge_gradient(grad, squares, minus_same, minus_cross, (minus_rest, relayed), -1, devices)
    partials = lax.all_to_all(spread, VOCAB_DP, 0, 0, tiled=True)
    return tuple(clipped_update(grad, own_table, partials, vocab_rows * width))


def solution(mesh):
    split = Mesh(
        mesh.devices.reshape(4, 4, 4, mesh.shape["dp"]), ("vocab_0", "vocab_1", "vocab_2", "dp")
    )
    return jax.shard_map(
        body,
        mesh=split,
        in_specs=(P(VOCAB, None), P("dp", VOCAB), P("dp", VOCAB, None)),
        out_specs=(P(VOCAB, "dp"), P()),
        check_vma=False,
    )
```

```python
import jax
import jax.numpy as jnp
from jax import lax
from jax.experimental import pallas as pl
from jax.experimental.pallas import tpu as pltpu
from jax.sharding import Mesh
from jax.sharding import PartitionSpec as P

VOCAB = ("vocab_0", "vocab_1", "vocab_2")
VOCAB_DP = ("vocab_0", "vocab_1", "vocab_2", "dp")
TOK_EDGE = 128
EDGE = 256
LANES = 128
TAIL = 16

step_rate = 0.5
norm_limit = 1.0


MIB = 1 << 20


def own_index():
    vocab = 0
    for name in VOCAB:
        vocab = vocab * lax.axis_size(name) + lax.axis_index(name)
    return vocab, lax.axis_index("dp")


def in_vmem(value):
    return pltpu.with_memory_space_constraint(value, pltpu.VMEM)


def in_hbm(value):
    return pltpu.with_memory_space_constraint(value, pltpu.HBM)


def any_spec():
    return pl.BlockSpec(memory_space=pltpu.HBM)


def vmem_spec():
    return pl.BlockSpec(memory_space=pltpu.VMEM)


def halves(value):
    high = lax.shift_right_logical(value, 8)
    low = jnp.bitwise_and(value, 255)
    return high.astype(jnp.float32), low.astype(jnp.float32)


def joined(high, low):
    return high.astype(jnp.int32) * 256 + low.astype(jnp.int32)


def pack(grad_rows, token_ids, rows_dev, vocab_rows, edges, swap):
    tokens, width = grad_rows.shape
    half = width // 2
    parts = 8

    def kernel(rows, ids_in, *refs):
        outs, (ids, sems) = refs[:-2], refs[-2:]
        vocab, core = own_index()
        copies = [pltpu.make_async_copy(ids_in, ids, sems.at[0])]
        for out, (at, crossed, first, count, _) in zip(outs, edges):
            columns = pl.multiple_of((1 - core if crossed else core) * half, half)
            for c in range(count):
                copies.append(
                    pltpu.make_async_copy(
                        rows.at[pl.ds(at, TOK_EDGE), pl.ds(columns + (first + c) * LANES, LANES)],
                        out.at[pl.ds(c * TOK_EDGE, TOK_EDGE), :],
                        sems.at[1],
                    )
                )
        if swap:
            columns = pl.multiple_of((1 - core) * half, half)
            step = tokens // parts
            for k in range(parts):
                copies.append(
                    pltpu.make_async_copy(
                        rows.at[pl.ds(k * step, step), pl.ds(columns, half)],
                        outs[-1].at[pl.ds(k * step, step), :],
                        sems.at[1],
                    )
                )
        for copy in copies:
            copy.start()
        copies[0].wait()
        offset = jnp.bitwise_and(ids[...] - vocab * rows_dev + EDGE, vocab_rows - 1)
        for out, (at, _, _, count, tail) in zip(outs, edges):
            if tail:
                high, low = halves(offset[:, at : at + TOK_EDGE])
                upper = lax.broadcasted_iota(jnp.int32, (TAIL, LANES), 0) < TAIL // 2
                out[pl.ds(count * TOK_EDGE, TAIL), :] = jnp.where(upper, high, low).astype(out.dtype)
        if swap:
            both = jnp.concatenate(halves(offset), axis=1)
            outs[-1][pl.ds(tokens, TAIL), :] = jnp.broadcast_to(both, (TAIL, half)).astype(grad_rows.dtype)
        for copy in copies[1:]:
            copy.wait()

    shapes = [
        pltpu.VMEM((count * TOK_EDGE + (TAIL if tail else 0), LANES), grad_rows.dtype)
        for _, _, _, count, tail in edges
    ]
    if swap:
        shapes.append(pltpu.VMEM((tokens + TAIL, half), grad_rows.dtype))
    return pl.pallas_call(
        kernel,
        out_shape=shapes,
        in_specs=[any_spec(), any_spec()],
        out_specs=[vmem_spec()] * len(shapes),
        scratch_shapes=[pltpu.VMEM((1, tokens), jnp.int32), pltpu.SemaphoreType.DMA((2,))],
        compiler_params=pltpu.CompilerParams(vmem_limit_bytes=8 * MIB),
    )(in_hbm(grad_rows), in_hbm(token_ids))


def local_gradient(grad_rows, swapped, own_ids, embed_table, vocab_rows):
    tokens, width = grad_rows.shape
    rows_dev = embed_table.shape[0]
    half = width // 2
    block = 256
    lanes = 512
    token_blocks = tokens // block
    row_blocks = rows_dev // block

    def kernel(rows, far_rows, ids_in, table, grad, own_table, squares, own_rows, ids, sems):
        vocab, core = own_index()
        own = pl.multiple_of(core * half, half)
        copies = [
            pltpu.make_async_copy(
                rows.at[pl.ds(k * block, block), pl.ds(own, half)], own_rows.at[pl.ds(k * block, block), :], sems.at[k]
            )
            for k in range(token_blocks)
        ]
        table_copies = [
            pltpu.make_async_copy(
                table.at[:, pl.ds(own + k * LANES, LANES)], own_table.at[k], sems.at[token_blocks]
            )
            for k in range(half // LANES)
        ]
        ids_copy = pltpu.make_async_copy(ids_in, ids, sems.at[token_blocks + 1])
        for copy in [ids_copy] + copies + table_copies:
            copy.start()
        for k in range(rows_dev // 64):
            grad[pl.ds(k * 64, 64), :] = jnp.zeros((64, half), jnp.float32)

        def accumulate(local, token_rows, ready):
            firsts = [local[0, k * block] for k in range(token_blocks)]
            for k in range(token_blocks):
                part = local[:, k * block : (k + 1) * block]
                low = jnp.maximum(lax.shift_right_arithmetic(firsts[k], 8), 0)
                high = row_blocks - 1
                if k + 1 < token_blocks:
                    high = jnp.minimum(lax.shift_right_arithmetic(firsts[k + 1], 8), high)
                ready(k)

                def step(r, carry):
                    base = pl.multiple_of(r * block, block)
                    at = lax.broadcasted_iota(jnp.int32, (block, block), 0) + base
                    hot = jnp.where(at == part, 1.0, 0.0).astype(jnp.bfloat16)
                    for c in range(half // lanes):
                        columns = pl.ds(c * lanes, lanes)
                        grad[pl.ds(base, block), columns] += jnp.dot(
                            hot, token_rows[pl.ds(k * block, block), columns], preferred_element_type=jnp.float32
                        )
                    return carry

                lax.fori_loop(low, high + 1, step, 0)

        sent = far_rows[pl.ds(tokens, TAIL), :].astype(jnp.float32)[:1, :]
        accumulate(joined(sent[:, :tokens], sent[:, tokens:]) - EDGE, far_rows, lambda k: None)
        ids_copy.wait()
        offset = jnp.bitwise_and(ids[...] - vocab * rows_dev + EDGE, vocab_rows - 1)
        accumulate(offset - EDGE, own_rows, lambda k: copies[k].wait())
        total = jnp.zeros((8, lanes), jnp.float32)
        for r in range(EDGE, rows_dev - EDGE, 64):
            for c in range(half // lanes):
                value = grad[pl.ds(r, 64), pl.ds(c * lanes, lanes)]
                total = total + jnp.sum((value * value).reshape(8, 8, lanes), axis=0)
        total = jnp.sum(total, axis=0, keepdims=True)
        fold = total[:, :LANES]
        for k in range(1, lanes // LANES):
            fold = fold + total[:, k * LANES : (k + 1) * LANES]
        squares[...] = fold
        for copy in table_copies:
            copy.wait()

    return pl.pallas_call(
        kernel,
        out_shape=[
            pltpu.VMEM((rows_dev, half), jnp.float32),
            pltpu.VMEM((half // LANES, rows_dev, LANES), embed_table.dtype),
            pltpu.VMEM((1, LANES), jnp.float32),
        ],
        in_specs=[any_spec(), vmem_spec(), any_spec(), any_spec()],
        out_specs=[vmem_spec()] * 3,
        scratch_shapes=[
            pltpu.VMEM((tokens, half), grad_rows.dtype),
            pltpu.VMEM((1, tokens), jnp.int32),
            pltpu.SemaphoreType.DMA((token_blocks + 2,)),
        ],
        compiler_params=pltpu.CompilerParams(vmem_limit_bytes=12 * MIB),
        cost_estimate=pl.CostEstimate(
            flops=4 * rows_dev * tokens * half, bytes_accessed=8 * MIB, transcendentals=0
        ),
        name="local_gradient",
    )(in_hbm(grad_rows), in_vmem(swapped), in_hbm(own_ids), in_hbm(embed_table))


def edge_gradient(grad, squares, same, cross, rest, side, tiles, spread_rows):
    rows_dev = grad.shape[0]
    group = 4
    base = rows_dev - EDGE if side < 0 else 0
    first = 0 if side < 0 else rows_dev + EDGE

    def kernel(grad_in, squares_in, same, cross, *refs):
        others, (grad_out, spread) = refs[:-2], refs[-2:]
        at = lax.broadcasted_iota(jnp.int32, (EDGE, TOK_EDGE), 0) + first
        hot = []
        for part in (same, cross):
            sent = part[pl.ds(part.shape[0] - TAIL, TAIL), :].astype(jnp.float32)
            offset = joined(sent[:1, :], sent[TAIL // 2 : TAIL // 2 + 1, :])
            hot.append(jnp.where(at == offset, 1.0, 0.0).astype(jnp.bfloat16))
        hot = jnp.concatenate(hot, axis=1)

        def same_tile(k):
            return same[pl.ds(k * TOK_EDGE, TOK_EDGE), :]

        def cross_tile(k):
            if not others:
                return cross[pl.ds(k * TOK_EDGE, TOK_EDGE), :]
            rows = pl.ds((k - tiles[0]) * TOK_EDGE, TOK_EDGE)
            return others[0][rows, :] + others[1][rows, :]

        total = jnp.zeros((8, LANES), jnp.float32)
        for low in range(tiles[0], tiles[1], group):
            span = range(low, min(low + group, tiles[1]))
            columns = pl.ds(low * LANES, len(span) * LANES)
            rows = jnp.concatenate(
                [
                    jnp.concatenate([tile(k) for k in span], axis=1)
                    for tile in (same_tile, cross_tile)
                ],
                axis=0,
            )
            value = grad_in[pl.ds(base, EDGE), columns] + jnp.dot(
                hot, rows, preferred_element_type=jnp.float32
            )
            grad_out[pl.ds(base, EDGE), columns] = value
            square = jnp.sum((value * value).reshape(EDGE // 8, 8, len(span) * LANES), axis=0)
            for k in range(len(span)):
                total = total + square[:, k * LANES : (k + 1) * LANES]
        fold = squares_in[...] + jnp.sum(total, axis=0, keepdims=True)
        spread[...] = jnp.broadcast_to(fold, (spread_rows, LANES))

    return pl.pallas_call(
        kernel,
        out_shape=[
            pltpu.VMEM(grad.shape, jnp.float32),
            pltpu.VMEM((spread_rows, LANES), jnp.float32),
        ],
        in_specs=[vmem_spec()] * (4 + len(rest)),
        out_specs=[vmem_spec()] * 2,
        input_output_aliases={0: 0},
        compiler_params=pltpu.CompilerParams(vmem_limit_bytes=4 * MIB),
        cost_estimate=pl.CostEstimate(
            flops=4 * EDGE * TOK_EDGE * (tiles[1] - tiles[0]) * LANES, bytes_accessed=2 * MIB, transcendentals=0
        ),
    )(in_vmem(grad), in_vmem(squares), in_vmem(same), in_vmem(cross), *[in_vmem(part) for part in rest])


def clipped_update(grad, own_table, partials, element_count):
    rows_dev, half = grad.shape
    tiles = half // LANES
    step = 64

    def kernel(grad_in, table_in, sums, updated, rms_out, stage, rms, sems):
        total = jnp.sum(jnp.sum(sums[...], axis=0, keepdims=True), axis=1, keepdims=True)
        grad_rms = jnp.sqrt(total / element_count)
        clip_scale = 1.0 / jnp.maximum(1.0, grad_rms / norm_limit)
        rate = step_rate * clip_scale
        rms[0] = grad_rms[0, 0]
        copies = [pltpu.make_async_copy(rms, rms_out, sems.at[tiles])]
        copies[0].start()
        for c in range(tiles):
            columns = pl.ds(c * LANES, LANES)
            for r in range(0, rows_dev, step):
                rows = pl.ds(r, step)
                stage[c, rows, :] = (
                    table_in[c, rows, :].astype(jnp.float32) - rate * grad_in[rows, columns]
                ).astype(stage.dtype)
            copies.append(pltpu.make_async_copy(stage.at[c], updated.at[:, columns], sems.at[c]))
            copies[-1].start()
        for copy in copies:
            copy.wait()

    return pl.pallas_call(
        kernel,
        out_shape=[
            jax.ShapeDtypeStruct((rows_dev, half), own_table.dtype),
            jax.ShapeDtypeStruct((1,), jnp.float32),
        ],
        in_specs=[vmem_spec()] * 3,
        out_specs=[any_spec(), any_spec()],
        scratch_shapes=[
            pltpu.VMEM((tiles, rows_dev, LANES), own_table.dtype),
            pltpu.SMEM((1,), jnp.float32),
            pltpu.SemaphoreType.DMA((tiles + 1,)),
        ],
        compiler_params=pltpu.CompilerParams(vmem_limit_bytes=8 * MIB),
        name="clipped_update",
    )(in_vmem(grad), in_vmem(own_table), in_vmem(partials))


def routes(vocab_count, replicas, step, flip, left_out=()):
    return [
        (v * replicas + p, (v + step) % vocab_count * replicas + (1 - p if flip else p))
        for v in range(vocab_count)
        for p in range(replicas)
        if v not in left_out
    ]


def body(embed_table, token_ids, grad_rows):
    rows_dev, width = embed_table.shape
    vocab_count = lax.axis_size(VOCAB)
    vocab_rows = rows_dev * vocab_count
    replicas = lax.axis_size("dp")
    devices = vocab_count * replicas
    rows = grad_rows[0]
    plane = vocab_count // lax.axis_size(VOCAB[0])
    line = lax.axis_size(VOCAB[2])
    corners = range(0, vocab_count, plane)
    relays = {}
    for v in corners:
        relays[v, 0] = (v + 2 * line - 1, 1)
        relays[v, 1] = ((v + plane + line - 1) % vocab_count, 0)
    to_relay = [(v * replicas + p, w * replicas + q) for (v, p), (w, q) in relays.items()]
    from_relay = [
        (w * replicas + q, (v - 1) % vocab_count * replicas + q) for (v, _), (w, q) in relays.items()
    ]

    def moved(piece, pairs):
        return lax.ppermute(piece, VOCAB_DP, pairs)

    def sent(piece, step, flip, left_out=()):
        return moved(piece, routes(vocab_count, replicas, step, flip, left_out))

    last = token_ids.shape[1] - TOK_EDGE
    tiles = width // replicas // LANES
    kept = tiles - 5
    shape = (rows_dev, vocab_rows)
    plus_same, minus_same, minus_rest = pack(
        rows,
        token_ids,
        *shape,
        (
            (last, False, 0, tiles, True),
            (0, False, 0, tiles, True),
            (0, True, kept, tiles - kept, False),
        ),
        False,
    )
    plus_same = sent(plus_same, 1, False)
    minus_same = sent(minus_same, -1, False)
    plus_cross, minus_cross, far = pack(
        rows, token_ids, *shape, ((last, True, 0, tiles, True), (0, True, 0, kept, True)), True
    )
    far = sent(far, 0, True)
    minus_cross = sent(minus_cross, -1, True)
    plus_cross = sent(plus_cross, 1, True)
    relayed = moved(minus_rest, to_relay)
    minus_rest = sent(minus_rest, -1, True, corners)
    relayed = moved(relayed, from_relay)
    grad, own_table, squares = local_gradient(rows, far, token_ids, embed_table, vocab_rows)
    grad, squares = edge_gradient(grad, squares, plus_same, plus_cross, (), 1, (0, tiles), 1)
    grad, squares = edge_gradient(grad, squares, minus_same, minus_cross, (), -1, (0, kept), 1)
    grad, spread = edge_gradient(
        grad, squares, minus_same, minus_cross, (minus_rest, relayed), -1, (kept, tiles), devices
    )
    partials = lax.all_to_all(spread, VOCAB_DP, 0, 0, tiled=True)
    return tuple(clipped_update(grad, own_table, partials, vocab_rows * width))


def solution(mesh):
    split = Mesh(
        mesh.devices.reshape(4, 4, 4, mesh.shape["dp"]), ("vocab_0", "vocab_1", "vocab_2", "dp")
    )
    return jax.shard_map(
        body,
        mesh=split,
        in_specs=(P(VOCAB, None), P("dp", VOCAB), P("dp", VOCAB, None)),
        out_specs=(P(VOCAB, "dp"), P()),
        check_vma=False,
    )
```

```python
import jax
import jax.numpy as jnp
from jax import lax
from jax.experimental import pallas as pl
from jax.experimental.pallas import tpu as pltpu
from jax.sharding import Mesh
from jax.sharding import PartitionSpec as P

VOCAB = ("vocab_0", "vocab_1", "vocab_2")
VOCAB_DP = ("vocab_0", "vocab_1", "vocab_2", "dp")
TOK_EDGE = 128
EDGE = 256
LANES = 128
TAIL = 16

step_rate = 0.5
norm_limit = 1.0


MIB = 1 << 20


def own_index():
    vocab = 0
    for name in VOCAB:
        vocab = vocab * lax.axis_size(name) + lax.axis_index(name)
    return vocab, lax.axis_index("dp")


def in_vmem(value):
    return pltpu.with_memory_space_constraint(value, pltpu.VMEM)


def in_hbm(value):
    return pltpu.with_memory_space_constraint(value, pltpu.HBM)


def any_spec():
    return pl.BlockSpec(memory_space=pltpu.HBM)


def vmem_spec():
    return pl.BlockSpec(memory_space=pltpu.VMEM)


def halves(value):
    high = lax.shift_right_logical(value, 8)
    low = jnp.bitwise_and(value, 255)
    return high.astype(jnp.float32), low.astype(jnp.float32)


def joined(high, low):
    return high.astype(jnp.int32) * 256 + low.astype(jnp.int32)


def pack(grad_rows, token_ids, rows_dev, vocab_rows, edges, swap):
    tokens, width = grad_rows.shape
    half = width // 2
    parts = 8

    def kernel(rows, ids_in, *refs):
        outs, (ids, sems) = refs[:-2], refs[-2:]
        vocab, core = own_index()
        copies = [pltpu.make_async_copy(ids_in, ids, sems.at[0])]
        for out, (at, crossed, first, count, _) in zip(outs, edges):
            columns = pl.multiple_of((1 - core if crossed else core) * half, half)
            for c in range(count):
                copies.append(
                    pltpu.make_async_copy(
                        rows.at[pl.ds(at, TOK_EDGE), pl.ds(columns + (first + c) * LANES, LANES)],
                        out.at[pl.ds(c * TOK_EDGE, TOK_EDGE), :],
                        sems.at[1],
                    )
                )
        if swap:
            columns = pl.multiple_of((1 - core) * half, half)
            step = tokens // parts
            for k in range(parts):
                copies.append(
                    pltpu.make_async_copy(
                        rows.at[pl.ds(k * step, step), pl.ds(columns, half)],
                        outs[-1].at[pl.ds(k * step, step), :],
                        sems.at[1],
                    )
                )
        for copy in copies:
            copy.start()
        copies[0].wait()
        offset = jnp.bitwise_and(ids[...] - vocab * rows_dev + EDGE, vocab_rows - 1)
        for out, (at, _, _, count, tail) in zip(outs, edges):
            if tail:
                high, low = halves(offset[:, at : at + TOK_EDGE])
                upper = lax.broadcasted_iota(jnp.int32, (TAIL, LANES), 0) < TAIL // 2
                out[pl.ds(count * TOK_EDGE, TAIL), :] = jnp.where(upper, high, low).astype(out.dtype)
        if swap:
            both = jnp.concatenate(halves(offset), axis=1)
            outs[-1][pl.ds(tokens, TAIL), :] = jnp.broadcast_to(both, (TAIL, half)).astype(grad_rows.dtype)
        for copy in copies[1:]:
            copy.wait()

    shapes = [
        pltpu.VMEM((count * TOK_EDGE + (TAIL if tail else 0), LANES), grad_rows.dtype)
        for _, _, _, count, tail in edges
    ]
    if swap:
        shapes.append(pltpu.VMEM((tokens + TAIL, half), grad_rows.dtype))
    return pl.pallas_call(
        kernel,
        out_shape=shapes,
        in_specs=[any_spec(), any_spec()],
        out_specs=[vmem_spec()] * len(shapes),
        scratch_shapes=[pltpu.VMEM((1, tokens), jnp.int32), pltpu.SemaphoreType.DMA((2,))],
        compiler_params=pltpu.CompilerParams(vmem_limit_bytes=8 * MIB),
    )(in_hbm(grad_rows), in_hbm(token_ids))


def local_gradient(grad_rows, swapped, own_ids, embed_table, vocab_rows):
    tokens, width = grad_rows.shape
    rows_dev = embed_table.shape[0]
    half = width // 2
    block = 256
    lanes = 512
    token_blocks = tokens // block
    row_blocks = rows_dev // block

    def kernel(rows, far_rows, ids_in, table, grad, own_table, squares, own_rows, ids, sems):
        vocab, core = own_index()
        own = pl.multiple_of(core * half, half)
        copies = [
            pltpu.make_async_copy(
                rows.at[pl.ds(k * block, block), pl.ds(own, half)], own_rows.at[pl.ds(k * block, block), :], sems.at[k]
            )
            for k in range(token_blocks)
        ]
        table_copies = [
            pltpu.make_async_copy(
                table.at[:, pl.ds(own + k * LANES, LANES)], own_table.at[k], sems.at[token_blocks]
            )
            for k in range(half // LANES)
        ]
        ids_copy = pltpu.make_async_copy(ids_in, ids, sems.at[token_blocks + 1])
        for copy in [ids_copy] + copies + table_copies:
            copy.start()
        for k in range(rows_dev // 64):
            grad[pl.ds(k * 64, 64), :] = jnp.zeros((64, half), jnp.float32)

        def accumulate(local, token_rows, ready):
            firsts = [local[0, k * block] for k in range(token_blocks)]
            for k in range(token_blocks):
                part = local[:, k * block : (k + 1) * block]
                low = jnp.maximum(lax.shift_right_arithmetic(firsts[k], 8), 0)
                high = row_blocks - 1
                if k + 1 < token_blocks:
                    high = jnp.minimum(lax.shift_right_arithmetic(firsts[k + 1], 8), high)
                ready(k)

                def step(r, carry):
                    base = pl.multiple_of(r * block, block)
                    at = lax.broadcasted_iota(jnp.int32, (block, block), 0) + base
                    hot = jnp.where(at == part, 1.0, 0.0).astype(jnp.bfloat16)
                    for c in range(half // lanes):
                        columns = pl.ds(c * lanes, lanes)
                        grad[pl.ds(base, block), columns] += jnp.dot(
                            hot, token_rows[pl.ds(k * block, block), columns], preferred_element_type=jnp.float32
                        )
                    return carry

                lax.fori_loop(low, high + 1, step, 0)

        sent = far_rows[pl.ds(tokens, TAIL), :].astype(jnp.float32)[:1, :]
        accumulate(joined(sent[:, :tokens], sent[:, tokens:]) - EDGE, far_rows, lambda k: None)
        ids_copy.wait()
        offset = jnp.bitwise_and(ids[...] - vocab * rows_dev + EDGE, vocab_rows - 1)
        accumulate(offset - EDGE, own_rows, lambda k: copies[k].wait())
        total = jnp.zeros((8, lanes), jnp.float32)
        for r in range(EDGE, rows_dev - EDGE, 64):
            for c in range(half // lanes):
                value = grad[pl.ds(r, 64), pl.ds(c * lanes, lanes)]
                total = total + jnp.sum((value * value).reshape(8, 8, lanes), axis=0)
        total = jnp.sum(total, axis=0, keepdims=True)
        fold = total[:, :LANES]
        for k in range(1, lanes // LANES):
            fold = fold + total[:, k * LANES : (k + 1) * LANES]
        squares[...] = fold
        for copy in table_copies:
            copy.wait()

    return pl.pallas_call(
        kernel,
        out_shape=[
            pltpu.VMEM((rows_dev, half), jnp.float32),
            pltpu.VMEM((half // LANES, rows_dev, LANES), embed_table.dtype),
            pltpu.VMEM((1, LANES), jnp.float32),
        ],
        in_specs=[any_spec(), vmem_spec(), any_spec(), any_spec()],
        out_specs=[vmem_spec()] * 3,
        scratch_shapes=[
            pltpu.VMEM((tokens, half), grad_rows.dtype),
            pltpu.VMEM((1, tokens), jnp.int32),
            pltpu.SemaphoreType.DMA((token_blocks + 2,)),
        ],
        compiler_params=pltpu.CompilerParams(vmem_limit_bytes=12 * MIB),
        cost_estimate=pl.CostEstimate(
            flops=4 * rows_dev * tokens * half, bytes_accessed=8 * MIB, transcendentals=0
        ),
        name="local_gradient",
    )(in_hbm(grad_rows), in_vmem(swapped), in_hbm(own_ids), in_hbm(embed_table))


def edge_gradient(grad, squares, same, cross, rest, side, tiles, spread_rows):
    rows_dev = grad.shape[0]
    group = 4
    base = rows_dev - EDGE if side < 0 else 0
    first = 0 if side < 0 else rows_dev + EDGE

    def kernel(grad_in, squares_in, same, cross, *refs):
        others, (grad_out, spread) = refs[:-2], refs[-2:]
        at = lax.broadcasted_iota(jnp.int32, (EDGE, TOK_EDGE), 0) + first
        hot = []
        for part in (same, cross):
            sent = part[pl.ds(part.shape[0] - TAIL, TAIL), :].astype(jnp.float32)
            offset = joined(sent[:1, :], sent[TAIL // 2 : TAIL // 2 + 1, :])
            hot.append(jnp.where(at == offset, 1.0, 0.0).astype(jnp.bfloat16))
        hot = jnp.concatenate(hot, axis=1)

        def same_tile(k):
            return same[pl.ds(k * TOK_EDGE, TOK_EDGE), :]

        def cross_tile(k):
            if not others:
                return cross[pl.ds(k * TOK_EDGE, TOK_EDGE), :]
            rows = pl.ds((k - tiles[0]) * TOK_EDGE, TOK_EDGE)
            return others[0][rows, :] + others[1][rows, :]

        total = jnp.zeros((8, LANES), jnp.float32)
        for low in range(tiles[0], tiles[1], group):
            span = range(low, min(low + group, tiles[1]))
            columns = pl.ds(low * LANES, len(span) * LANES)
            rows = jnp.concatenate(
                [
                    jnp.concatenate([tile(k) for k in span], axis=1)
                    for tile in (same_tile, cross_tile)
                ],
                axis=0,
            )
            value = grad_in[pl.ds(base, EDGE), columns] + jnp.dot(
                hot, rows, preferred_element_type=jnp.float32
            )
            grad_out[pl.ds(base, EDGE), columns] = value
            square = jnp.sum((value * value).reshape(EDGE // 8, 8, len(span) * LANES), axis=0)
            for k in range(len(span)):
                total = total + square[:, k * LANES : (k + 1) * LANES]
        fold = squares_in[...] + jnp.sum(total, axis=0, keepdims=True)
        spread[...] = jnp.broadcast_to(fold, (spread_rows, LANES))

    return pl.pallas_call(
        kernel,
        out_shape=[
            pltpu.VMEM(grad.shape, jnp.float32),
            pltpu.VMEM((spread_rows, LANES), jnp.float32),
        ],
        in_specs=[vmem_spec()] * (4 + len(rest)),
        out_specs=[vmem_spec()] * 2,
        input_output_aliases={0: 0},
        compiler_params=pltpu.CompilerParams(vmem_limit_bytes=4 * MIB),
        cost_estimate=pl.CostEstimate(
            flops=4 * EDGE * TOK_EDGE * (tiles[1] - tiles[0]) * LANES, bytes_accessed=2 * MIB, transcendentals=0
        ),
    )(in_vmem(grad), in_vmem(squares), in_vmem(same), in_vmem(cross), *[in_vmem(part) for part in rest])


def clipped_update(grad, own_table, partials, element_count):
    rows_dev, half = grad.shape
    tiles = half // LANES
    step = 64

    def kernel(grad_in, table_in, sums, updated, rms_out, stage, rms, sems):
        total = jnp.sum(jnp.sum(sums[...], axis=0, keepdims=True), axis=1, keepdims=True)
        grad_rms = jnp.sqrt(total / element_count)
        clip_scale = 1.0 / jnp.maximum(1.0, grad_rms / norm_limit)
        rate = step_rate * clip_scale
        rms[0] = grad_rms[0, 0]
        copies = [pltpu.make_async_copy(rms, rms_out, sems.at[tiles])]
        copies[0].start()
        for c in range(tiles):
            columns = pl.ds(c * LANES, LANES)
            for r in range(0, rows_dev, step):
                rows = pl.ds(r, step)
                stage[c, rows, :] = (
                    table_in[c, rows, :].astype(jnp.float32) - rate * grad_in[rows, columns]
                ).astype(stage.dtype)
            copies.append(pltpu.make_async_copy(stage.at[c], updated.at[:, columns], sems.at[c]))
            copies[-1].start()
        for copy in copies:
            copy.wait()

    return pl.pallas_call(
        kernel,
        out_shape=[
            jax.ShapeDtypeStruct((rows_dev, half), own_table.dtype),
            jax.ShapeDtypeStruct((1,), jnp.float32),
        ],
        in_specs=[vmem_spec()] * 3,
        out_specs=[any_spec(), any_spec()],
        scratch_shapes=[
            pltpu.VMEM((tiles, rows_dev, LANES), own_table.dtype),
            pltpu.SMEM((1,), jnp.float32),
            pltpu.SemaphoreType.DMA((tiles + 1,)),
        ],
        compiler_params=pltpu.CompilerParams(vmem_limit_bytes=8 * MIB),
        name="clipped_update",
    )(in_vmem(grad), in_vmem(own_table), in_vmem(partials))


def routes(vocab_count, replicas, step, flip, left_out=()):
    return [
        (v * replicas + p, (v + step) % vocab_count * replicas + (1 - p if flip else p))
        for v in range(vocab_count)
        for p in range(replicas)
        if v not in left_out
    ]


def body(embed_table, token_ids, grad_rows):
    rows_dev, width = embed_table.shape
    vocab_count = lax.axis_size(VOCAB)
    vocab_rows = rows_dev * vocab_count
    replicas = lax.axis_size("dp")
    devices = vocab_count * replicas
    rows = grad_rows[0]
    plane = vocab_count // lax.axis_size(VOCAB[0])
    line = lax.axis_size(VOCAB[2])
    corners = range(0, vocab_count, plane)
    relays = {}
    for v in corners:
        relays[v, 0] = (v + 2 * line - 1, 1)
        relays[v, 1] = ((v + plane + line - 1) % vocab_count, 0)
    to_relay = [(v * replicas + p, w * replicas + q) for (v, p), (w, q) in relays.items()]
    from_relay = [
        (w * replicas + q, (v - 1) % vocab_count * replicas + q) for (v, _), (w, q) in relays.items()
    ]

    def moved(piece, pairs):
        return lax.ppermute(piece, VOCAB_DP, pairs)

    def sent(piece, step, flip, left_out=()):
        return moved(piece, routes(vocab_count, replicas, step, flip, left_out))

    last = token_ids.shape[1] - TOK_EDGE
    tiles = width // replicas // LANES
    kept = tiles - 5
    shape = (rows_dev, vocab_rows)
    plus_same, minus_same = pack(
        rows,
        token_ids,
        *shape,
        (
            (last, False, 0, tiles, True),
            (0, False, 0, tiles, True),
        ),
        False,
    )
    plus_same = sent(plus_same, 1, False)
    minus_same = sent(minus_same, -1, False)
    plus_cross, minus_cross, minus_rest, far = pack(
        rows,
        token_ids,
        *shape,
        ((last, True, 0, tiles, True), (0, True, 0, kept, True), (0, True, kept, tiles - kept, False)),
        True,
    )
    far = sent(far, 0, True)
    minus_cross = sent(minus_cross, -1, True)
    plus_cross = sent(plus_cross, 1, True)
    relayed = moved(minus_rest, to_relay)
    minus_rest = sent(minus_rest, -1, True, corners)
    relayed = moved(relayed, from_relay)
    grad, own_table, squares = local_gradient(rows, far, token_ids, embed_table, vocab_rows)
    grad, squares = edge_gradient(grad, squares, plus_same, plus_cross, (), 1, (0, tiles), 1)
    grad, squares = edge_gradient(grad, squares, minus_same, minus_cross, (), -1, (0, kept), 1)
    grad, spread = edge_gradient(
        grad, squares, minus_same, minus_cross, (minus_rest, relayed), -1, (kept, tiles), devices
    )
    partials = lax.all_to_all(spread, VOCAB_DP, 0, 0, tiled=True)
    return tuple(clipped_update(grad, own_table, partials, vocab_rows * width))


def solution(mesh):
    split = Mesh(
        mesh.devices.reshape(4, 4, 4, mesh.shape["dp"]), ("vocab_0", "vocab_1", "vocab_2", "dp")
    )
    return jax.shard_map(
        body,
        mesh=split,
        in_specs=(P(VOCAB, None), P("dp", VOCAB), P("dp", VOCAB, None)),
        out_specs=(P(VOCAB, "dp"), P()),
        check_vma=False,
    )
```
